512 devices in a mesh: pool: 16 (over y, core), ga: 32 (over x, z).
Axes of the slice: x: 4, y: 8, z: 8, core: 2. Of those that a mesh axis runs over, the one named last changes fastest.
Arguments:
- coefficients: bfloat16 [16, 1024, 2, 256, 128], P('pool', 'ga'), may hold values from -6 to 6
- stick_count: int32 [16, 32], P('pool', 'ga'), may hold values from 28 to 32, as said below
- dest_device: int32 [16, 1024], P('pool', 'ga'), may hold values from -1 to 31, as said below
- dest_slot: int32 [16, 1024], P('pool', 'ga'), may hold values from -1 to 31, as said below
- source_stick: int32 [16, 1024], P('pool', 'ga'), may hold values from -1 to 1023, as said below
Outputs:
- margins: float32 [16, 2, 256, 256], P('pool', None, 'ga')
The draws below stay inside these ranges and needn't reach their ends.
Inputs may be any that keep to these rules, and one draw needn't show every extreme that they name: Every k-point has a device whose 32 slots are all live; a device's live sticks are its first stick_count slots. `dest_device`: -1 exactly for sticks that land nowhere (among them all sticks that are not live); no device sends more than 2 of its sticks to one device, and some pair of devices reaches 2 for every k-point. `dest_slot`: -1 where dest_device is -1; the slots named are live slots of the layout of k-point q-1, no slot named twice. `source_stick`: the exact inverse of dest_device and dest_slot: a slot names a stick exactly when that stick names the slot, else -1.
All inputs are finite; a program needn't handle non-finite values.
Results may differ from the reference program's by a relative error of at most 0.0003.
Values may be sent and summed in bfloat16 or wider, within the bound.
A program may use at most 64 MiB of HBM per device.

```python
import jax
import jax.numpy as jnp
from jax import lax

NB = 256
PW = 128
SLOTS = 32
KPTS = 16
STICKS = 1024
CAP = 2
N_GA = 32


def stick_maps(key):
    base_key = jax.random.fold_in(key, 7101)
    subkeys = jax.random.split(base_key, 6)
    lowest = SLOTS - max(1, SLOTS // 8)
    counts = jax.random.randint(subkeys[0], (KPTS, N_GA), lowest, SLOTS + 1)
    shifts = jax.random.randint(subkeys[1], (KPTS,), 0, N_GA)
    offsets = jax.vmap(lambda sub: jax.random.permutation(sub, N_GA))(jax.random.split(subkeys[2], KPTS))
    dest_order = jax.vmap(lambda sub: jax.random.permutation(sub, SLOTS))(jax.random.split(subkeys[3], KPTS * N_GA)).reshape(KPTS, N_GA, SLOTS)
    source_order = jax.vmap(lambda sub: jax.random.permutation(sub, SLOTS))(jax.random.split(subkeys[4], KPTS * N_GA)).reshape(KPTS, N_GA, SLOTS)
    full_dest = jax.random.randint(subkeys[5], (KPTS,), 0, N_GA)
    kpoint_list = jnp.arange(KPTS)
    counts = counts.at[(kpoint_list - 1) % KPTS, full_dest].set(SLOTS)
    full_source = (full_dest + shifts + offsets[:, 0]) % N_GA
    counts = counts.at[kpoint_list, full_source].set(SLOTS)
    shape = (KPTS, N_GA, SLOTS)
    device_grid = jnp.broadcast_to(jnp.arange(N_GA)[None, :, None], shape)
    kpoint_grid = jnp.broadcast_to(kpoint_list[:, None, None], shape)
    block_of = jnp.arange(SLOTS) // CAP
    chosen = offsets[:, block_of][:, None, :]
    source_dev = (device_grid + shifts[:, None, None] + chosen) % N_GA
    source_slot = jnp.take_along_axis(source_order, source_dev, axis=1)
    prev_counts = jnp.roll(counts, 1, axis=0)
    dest_live = dest_order < prev_counts[:, :, None]
    source_counts = jnp.take_along_axis(counts, source_dev.reshape(KPTS, N_GA * SLOTS), axis=1).reshape(shape)
    source_live = source_slot < source_counts
    valid = dest_live & source_live
    empty = jnp.full(shape, -1, jnp.int32)
    source_stick = empty.at[kpoint_grid, device_grid, dest_order].set(jnp.where(valid, source_dev * SLOTS + source_slot, -1).astype(jnp.int32))
    dest_device = empty.at[kpoint_grid, source_dev, source_slot].set(jnp.where(valid, device_grid, -1).astype(jnp.int32))
    dest_slot = empty.at[kpoint_grid, source_dev, source_slot].set(jnp.where(valid, dest_order, -1).astype(jnp.int32))
    flat_shape = (KPTS, N_GA * SLOTS)
    return (counts.astype(jnp.int32), dest_device.reshape(flat_shape), dest_slot.reshape(flat_shape), source_stick.reshape(flat_shape))


def draw_stick_count(key, part):
    return stick_maps(key)[0]


def draw_dest_device(key, part):
    return stick_maps(key)[1]


def draw_dest_slot(key, part):
    return stick_maps(key)[2]


def draw_source_stick(key, part):
    return stick_maps(key)[3]


def block_scale(own_key, dims, cuts, low, top_value):
    def one(position, shards_of):
        heights = jax.random.uniform(jax.random.fold_in(jax.random.fold_in(own_key, 6), position), (shards_of,), jnp.float32, low / len(cuts), top_value / len(cuts))
        return jnp.repeat(jnp.exp(heights), dims[position] // shards_of).reshape((-1,) + (1,) * (len(dims) - position - 1))

    gain = one(*cuts[0])
    for cut in cuts[1:]:
        gain = gain * one(*cut)
    return gain


def noise(own_key, extent, width, bound, pieces=(), kind=jnp.bfloat16):
    array = jax.random.normal(own_key, extent, jnp.float32) * width
    if len(pieces) > 0:
        array = block_scale(own_key, extent, pieces, -0.22, 0.18) * array
    return jnp.clip(array, min=-bound, max=bound).astype(kind)


def setup_inputs(seed: int = 0) -> dict:
    streams_of = jax.random.split(jax.random.key(seed), 6)
    coefficients = noise(streams_of[0], (KPTS, STICKS, 2, NB, PW), 1.0, 6.0, ((0, 16), (1, 32)))
    stick_count = draw_stick_count(jax.random.fold_in(streams_of[5], 71), 0)
    dest_device = draw_dest_device(jax.random.fold_in(streams_of[5], 71), 0)
    dest_slot = draw_dest_slot(jax.random.fold_in(streams_of[5], 71), 0)
    source_stick = draw_source_stick(jax.random.fold_in(streams_of[5], 71), 0)
    return {"coefficients": coefficients, "stick_count": stick_count, "dest_device": dest_device, "dest_slot": dest_slot, "source_stick": source_stick}


def reference(coefficients, stick_count, dest_device, dest_slot, source_stick):
    norm_scale = jnp.float32((2 * STICKS * PW) ** -0.5)
    slot_index = (jnp.arange(STICKS) % SLOTS).astype(jnp.int32)
    owner_device = (jnp.arange(STICKS) // SLOTS).astype(jnp.int32)
    results = []
    for kpoint in range(KPTS):
        neighbour = (kpoint + 1) % KPTS
        live_mask = slot_index < stick_count[kpoint][owner_device]
        bra_rows = jnp.where(live_mask[:, None, None, None], coefficients[kpoint], 0).astype(jnp.float32)
        anchor = source_stick[neighbour]
        safe_index = jnp.clip(anchor, 0, STICKS - 1).astype(jnp.int32)
        agreeing = (anchor >= 0) & (dest_device[neighbour][safe_index] == owner_device) & (dest_slot[neighbour][safe_index] == slot_index)
        ket_rows = jnp.where(agreeing[:, None, None, None], coefficients[neighbour][safe_index], 0).astype(jnp.float32)
        swapped = jnp.stack([ket_rows[:, 1], -ket_rows[:, 0]], axis=1)
        real_part = jnp.einsum('scmg,scng->mn', bra_rows, ket_rows, precision=lax.Precision.HIGHEST)
        imag_part = jnp.einsum('scmg,scng->mn', bra_rows, swapped, precision=lax.Precision.HIGHEST)
        results.append(jnp.stack([real_part, imag_part]) * norm_scale)
    return jnp.stack(results)
```

```python
import functools

import jax
import jax.numpy as jnp
from jax import lax
from jax.experimental import pallas as pl
from jax.experimental.pallas import tpu as pltpu
from jax.sharding import PartitionSpec as P

MESH = pl.DeviceIdType.MESH
NX = 4
NZ = 8
WINDOW = 5


def hop_list():
    far = []
    for distance, hop in ((4, 1), (3, 1), (1, 1), (2, 1), (4, 2), (3, 2), (2, 2), (4, 3), (3, 3), (4, 4)):
        far += [(distance, hop, dx) for dx in (2, 1, 3)]
    near = [(d, h, 0) for d, h in ((4, 1), (3, 1), (2, 1), (4, 2), (3, 2), (2, 2), (4, 3), (3, 3), (4, 4), (1, 1))]
    return far + near


HOPS = hop_list()
RELAY = {(2, 1): 0, (3, 1): 1, (3, 2): 2}


def kernel(
    norm_scale,
    pack_ref,
    place_ref,
    count_ref,
    coef_hbm,
    out_ref,
    coef,
    bra,
    count_in,
    packed,
    relay,
    relay_half,
    turn,
    final,
    acc,
    x_in,
    rows,
    z_in,
    load_sem,
    bra_sem,
    count_sem,
    hop_send,
    hop_recv,
    x_send,
    x_recv,
    xr_send,
    xr_recv,
    zr_send,
    zr_recv,
):
    pool = lax.axis_index("pool")
    pools = lax.axis_size("pool")
    ga = lax.axis_index("ga")
    x = ga // NZ
    z = lax.rem(ga, NZ)
    after = lax.rem(pool + 1, pools)
    before = lax.rem(pool + pools - 1, pools)

    def at(dx, dz):
        return lax.rem(x + dx, NX) * NZ + lax.rem(z + dz, NZ)

    load = pltpu.make_async_copy(coef_hbm, coef, load_sem)
    load.start()
    barrier = pltpu.get_barrier_semaphore()
    greeted = [(pool, at(0, 1)), (pool, at(0, NZ - 1))]
    greeted += [(pool, at(dx, 0)) for dx in range(1, NX)]
    greeted += [(before, ga)] + [(after, at(0, dz)) for dz in range(NZ)]
    for device in greeted:
        pl.semaphore_signal(barrier, inc=1, device_id=device, device_id_type=MESH)

    load.wait()

    def pack_unit(unit, carry):
        target = at(lax.rem(unit, NX), unit // NX)
        for rank in range(2):
            packed[unit, rank] = coef[pack_ref[target * 2 + rank]]
        return carry

    lax.fori_loop(0, NX * NZ, pack_unit, 0)
    final[0] = packed[0]
    acc[...] = jnp.zeros_like(acc)
    pl.semaphore_wait(barrier, len(greeted))

    def remote(src, dst, send, recv, device):
        return pltpu.make_async_remote_copy(
            src_ref=src, dst_ref=dst, send_sem=send, recv_sem=recv, device_id=device, device_id_type=MESH
        )

    started = []

    def start(copy):
        copy.start()
        started.append(copy)
        return copy

    def hop_copy(s, n):
        distance, hop, dx = HOPS[n]
        dz = distance if s == 0 else NZ - distance
        unit = dz * NX + dx
        half = distance == NZ // 2
        if hop == 1:
            src = packed.at[unit, s] if half else packed.at[unit]
        elif half:
            src = relay_half.at[s, hop - 2, dx]
        else:
            src = relay.at[s, RELAY[distance, hop - 1], dx]
        if hop < distance:
            dst = relay_half.at[s, hop - 1, dx] if half else relay.at[s, RELAY[distance, hop], dx]
        else:
            dst = final.at[unit] if dx == 0 else turn.at[(dz - 1) * 3 + dx - 1]
            dst = dst.at[s] if half else dst
        return remote(src, dst, hop_send.at[s, n], hop_recv.at[s, n], (pool, at(0, 1 if s == 0 else NZ - 1)))

    hop_copies = [[hop_copy(s, n) for n in range(len(HOPS))] for s in range(2)]

    def x_copy(dz, dx, s):
        unit = dz * NX + dx
        src = packed.at[unit] if dz == 0 else turn.at[(dz - 1) * 3 + dx - 1]
        dst = final.at[unit]
        if dz == NZ // 2:
            src, dst = src.at[s], dst.at[s]
        return remote(src, dst, x_send.at[unit, s], x_recv.at[unit, s], (pool, at(dx, 0)))

    x_copies = {}

    def multiply(first, count, step):
        def one(i, carry):
            unit = first + i * step
            source = lax.rem(x + NX - lax.rem(unit, NX), NX) * NZ + lax.rem(z + NZ - unit // NX, NZ)
            total = None
            for rank in range(2):
                slot = place_ref[source * 2 + rank]
                live = (slot >= 0) & (slot < count_in[0, 0])
                mine = bra[jnp.maximum(slot, 0)]
                mine = jnp.where(live, mine, jnp.zeros_like(mine))
                ket = final[unit, rank]
                ket = jnp.concatenate([ket[:256], ket[256:]], axis=1)
                re, im = mine[:256], mine[256:]
                left = jnp.concatenate(
                    [jnp.concatenate([re, im], axis=1), jnp.concatenate([-im, re], axis=1)], axis=0
                )
                term = lax.dot_general(left, ket, (((1,), (1,)), ((), ())), preferred_element_type=jnp.float32)
                total = term if total is None else total + term
            acc[...] += total.reshape(acc.shape)
            return carry

        lax.fori_loop(0, count, one, 0)

    issued = [0, 0]
    position = {hop: n for n, hop in enumerate(HOPS)}

    def issue(s, arrived):
        while issued[s] < len(HOPS) and issued[s] <= arrived + WINDOW:
            distance, hop, dx = HOPS[issued[s]]
            if hop > 1 and position[distance, hop - 1, dx] > arrived:
                break
            start(hop_copies[s][issued[s]])
            issued[s] += 1

    for s in range(2):
        issue(s, -1)
    bra_copy = start(remote(coef, bra, bra_sem.at[0], bra_sem.at[1], (after, ga)))
    count_copy = start(remote(count_ref, count_in, count_sem.at[0], count_sem.at[1], (after, ga)))
    for dx in (2, 1, 3):
        x_copies[0, dx, 0] = start(x_copy(0, dx, 0))

    def wait_x(*units):
        for key in units:
            x_copies[key].wait_recv()

    three = (2, 1, 3)
    for n, (distance, hop, dx) in enumerate(HOPS):
        for s in range(2):
            hop_copies[s][n].wait_recv()
            if hop == distance and dx != 0:
                dz = distance if s == 0 else NZ - distance
                which = s if distance == NZ // 2 else 0
                x_copies[dz, dx, which] = start(x_copy(dz, dx, which))
            issue(s, n)
        if n == 11:
            bra_copy.wait_recv()
            count_copy.wait_recv()
            wait_x(*[(0, d, 0) for d in three])
            multiply(0, 4, 1)
        if n == 16:
            wait_x(*[(dz, d, 0) for dz in (1, 7) for d in three])
            multiply(5, 3, 1)
            multiply(29, 3, 1)
        if n == 26:
            wait_x(*[(dz, d, 0) for dz in (2, 6) for d in three])
            multiply(9, 3, 1)
            multiply(25, 3, 1)
        if n == 32:
            wait_x(*[(dz, d, 0) for dz in (3, 5) for d in three])
            multiply(13, 3, 1)
            multiply(21, 3, 1)
        if n == 35:
            wait_x(*[(4, d, h) for h in range(2) for d in three])
            multiply(17, 3, 1)
        if n == 37:
            multiply(8, 2, 16)
        if n == 38:
            multiply(12, 3, 4)
    multiply(4, 2, 24)

    sums = []
    for dx in (2, 1, 3):
        theirs = pl.ds(pl.multiple_of(lax.rem(x + dx, NX) * 64, 64), 64)
        sums.append(
            start(
                remote(
                    acc.at[:, theirs], x_in.at[dx - 1], xr_send.at[dx - 1], xr_recv.at[dx - 1], (pool, at(dx, 0))
                )
            )
        )
    for copy in sums:
        copy.wait_recv()
    own = pl.ds(pl.multiple_of(x * 64, 64), 64)
    rows[...] = acc[:, own] + x_in[0] + x_in[1] + x_in[2]
    sums = []
    for dz in (4, 3, 5, 2, 6, 1, 7, 0):
        theirs = pl.ds(pl.multiple_of(lax.rem(z + dz, NZ) * 8, 8), 8)
        sums.append(
            start(remote(rows.at[:, theirs], z_in.at[dz], zr_send.at[dz], zr_recv.at[dz], (before, at(0, dz))))
        )
    for copy in sums:
        copy.wait_recv()
    result = z_in[0]
    for dz in range(1, NZ):
        result = result + z_in[dz]
    out_ref[...] = result * norm_scale
    for copy in started:
        copy.wait_send()


def local(coefficients, stick_count, dest_device, dest_slot, source_stick):
    groups = lax.axis_size("ga")
    slots = coefficients.shape[1]
    bands = coefficients.shape[3]
    waves = coefficients.shape[4]
    norm_scale = (2 * groups * slots * waves) ** (-0.5)
    slot_list = jnp.arange(slots, dtype=jnp.int32)
    row_list = jnp.arange(groups * 2, dtype=jnp.int32)

    def ranked(devices, order):
        same = (devices[:, None] == devices[None, :]) & (order[None, :] < order[:, None])
        rank = jnp.sum(same.astype(jnp.int32), axis=1)
        return jnp.where(devices >= 0, devices * 2 + rank, -1)

    sent = row_list[:, None] == ranked(dest_device[0], dest_slot[0])[None, :]
    pack = jnp.max(jnp.where(sent, slot_list[None, :], 0), axis=1)
    anchor = source_stick[0]
    came = row_list[:, None] == ranked(jnp.where(anchor >= 0, anchor // slots, -1), slot_list)[None, :]
    place = jnp.max(jnp.where(came, slot_list[None, :], -1), axis=1)
    count = jnp.broadcast_to(stick_count, (8, 128))

    stick = (2 * bands, waves)
    bf16, f32 = jnp.bfloat16, jnp.float32
    dma = pltpu.SemaphoreType.DMA
    result = pl.pallas_call(
        functools.partial(kernel, norm_scale),
        out_shape=jax.ShapeDtypeStruct((2, bands // groups, bands), f32),
        in_specs=[
            pl.BlockSpec(memory_space=pltpu.SMEM),
            pl.BlockSpec(memory_space=pltpu.SMEM),
            pl.BlockSpec(memory_space=pltpu.VMEM),
            pl.BlockSpec(memory_space=pl.ANY),
        ],
        out_specs=pl.BlockSpec(memory_space=pltpu.VMEM),
        scratch_shapes=[
            pltpu.VMEM((slots,) + stick, bf16),
            pltpu.VMEM((slots,) + stick, bf16),
            pltpu.VMEM((8, 128), jnp.int32),
            pltpu.VMEM((NX * NZ, 2) + stick, bf16),
            pltpu.VMEM((2, 3, NX, 2) + stick, bf16),
            pltpu.VMEM((2, 3, NX) + stick, bf16),
            pltpu.VMEM((3 * (NZ - 1), 2) + stick, bf16),
            pltpu.VMEM((NX * NZ, 2) + stick, bf16),
            pltpu.VMEM((2, bands, bands), f32),
            pltpu.VMEM((NX - 1, 2, bands // NX, bands), f32),
            pltpu.VMEM((2, bands // NX, bands), f32),
            pltpu.VMEM((NZ, 2, bands // groups, bands), f32),
            dma,
            dma((2,)),
            dma((2,)),
            dma((2, len(HOPS))),
            dma((2, len(HOPS))),
            dma((NX * NZ, 2)),
            dma((NX * NZ, 2)),
            dma((NX - 1,)),
            dma((NX - 1,)),
            dma((NZ,)),
            dma((NZ,)),
        ],
        compiler_params=pltpu.CompilerParams(
            collective_id=0, has_side_effects=True, vmem_limit_bytes=56 * 2**20
        ),
    )(pack, place, count, coefficients.reshape((slots,) + stick))
    return result[None]


def solution(mesh):
    return jax.shard_map(
        local,
        mesh=mesh,
        in_specs=(
            P("pool", "ga", None, None, None),
            P("pool", "ga"),
            P("pool", "ga"),
            P("pool", "ga"),
            P("pool", "ga"),
        ),
        out_specs=P("pool", None, "ga", None),
        check_vma=False,
    )
```

```python
import functools

import jax
import jax.numpy as jnp
from jax import lax
from jax.experimental import pallas as pl
from jax.experimental.pallas import tpu as pltpu
from jax.sharding import PartitionSpec as P

MESH = pl.DeviceIdType.MESH
NX = 4
NZ = 8
WINDOW = 6
GROUP = 64
PARTS = ((0, 192), (192, 64))


def hop_list():
    order = []

    def add(part, dxs, *hops):
        order.extend((part, distance, hop, dx) for distance, hop in hops for dx in dxs)

    far = (2, 1, 3)
    add(0, far, (4, 1), (3, 1), (1, 1), (2, 1), (4, 2), (3, 2), (2, 2), (4, 3), (3, 3), (4, 4))
    add(0, (0,), (4, 1), (3, 1), (2, 1), (4, 2), (3, 2), (2, 2), (4, 3), (3, 3), (4, 4), (1, 1))
    add(1, far, (1, 1), (4, 1), (3, 1), (2, 1), (4, 2), (3, 2), (2, 2))
    add(1, (0,), (4, 1))
    add(1, far, (4, 3))
    add(1, (0,), (3, 1))
    add(1, far, (3, 3))
    add(1, (0,), (4, 2), (3, 2))
    add(1, far, (4, 4))
    add(1, (0,), (2, 1), (4, 3), (3, 3), (1, 1), (2, 2), (4, 4))
    return order


HOPS = hop_list()
RELAY = {(2, 1): 0, (3, 1): 1, (3, 2): 2}


def kernel(
    norm_scale,
    coef_hbm,
    count_hbm,
    device_hbm,
    slot_hbm,
    source_hbm,
    out_ref,
    coef,
    bra,
    maps,
    tables,
    table,
    count_out,
    count_in,
    packed,
    relay,
    relay_half,
    turn,
    final,
    acc,
    x_in,
    rows,
    z_in,
    tail_in,
    load_sem,
    map_sem,
    table_sem,
    bra_sem,
    count_sem,
    hop_send,
    hop_recv,
    x_send,
    x_recv,
    xr_send,
    xr_recv,
    zr_send,
    zr_recv,
    tail_send,
    tail_recv,
):
    pool = lax.axis_index("pool")
    pools = lax.axis_size("pool")
    ga = lax.axis_index("ga")
    x = ga // NZ
    z = lax.rem(ga, NZ)
    after = lax.rem(pool + 1, pools)
    before = lax.rem(pool + pools - 1, pools)

    def at(dx, dz):
        return lax.rem(x + dx, NX) * NZ + lax.rem(z + dz, NZ)

    small = []
    for i, ref in enumerate((device_hbm, slot_hbm, source_hbm, count_hbm)):
        small.append(pltpu.make_async_copy(ref, maps[i], map_sem.at[i]))
        small[-1].start()
    load = pltpu.make_async_copy(coef_hbm, coef, load_sem)
    load.start()
    barrier = pltpu.get_barrier_semaphore()
    greeted = [(pool, at(0, 1)), (pool, at(0, NZ - 1))]
    greeted += [(pool, at(dx, 0)) for dx in range(1, NX)]
    greeted += [(before, ga)] + [(after, at(dx, dz)) for dz in range(NZ) for dx in range(NX)]
    for device in greeted:
        pl.semaphore_signal(barrier, inc=1, device_id=device, device_id_type=MESH)

    for copy in small:
        copy.wait()
    sent = maps[0][...]
    from_stick = maps[2][...]
    slots = sent.shape[1]
    upright = lax.broadcasted_iota(jnp.int32, (slots, slots), 0)
    across = lax.broadcasted_iota(jnp.int32, (slots, slots), 1)

    def standing(row):
        return jnp.sum(jnp.where(upright == across, row, 0), axis=1, keepdims=True)

    def rows_of(devices, order, missing):
        device, key = standing(devices), standing(order)
        earlier = (device == devices) & (order < key)
        rank = jnp.sum(earlier.astype(jnp.int32), axis=1, keepdims=True)
        row = jnp.where(device >= 0, device * 2 + rank, -1)
        lane = lax.broadcasted_iota(jnp.int32, (slots, 128), 1)
        stick = lax.broadcasted_iota(jnp.int32, (slots, 128), 0)
        return jnp.max(jnp.where(row == lane, stick, missing), axis=0, keepdims=True)

    tables[0:1] = rows_of(sent, maps[1][...], 0)
    tables[1:2] = rows_of(
        jnp.where(from_stick >= 0, from_stick // slots, -1), across[:1], -1
    )
    count_out[...] = jnp.broadcast_to(maps[3][...], count_out.shape)
    for total in acc:
        total[...] = jnp.zeros_like(total)
    to_scalars = pltpu.make_async_copy(tables, table, table_sem)
    to_scalars.start()
    load.wait()
    to_scalars.wait()

    def pack_unit(unit, carry):
        target = at(lax.rem(unit, NX), unit // NX)
        for rank in range(2):
            stick = coef[table[0, target * 2 + rank]]
            for part, (first, bands) in enumerate(PARTS):
                packed[part][unit, rank] = stick[:, first : first + bands]
        return carry

    lax.fori_loop(12, 24, pack_unit, 0)
    pl.semaphore_wait(barrier, len(greeted))

    def remote(src, dst, send, recv, device):
        return pltpu.make_async_remote_copy(
            src_ref=src, dst_ref=dst, send_sem=send, recv_sem=recv, device_id=device, device_id_type=MESH
        )

    started = []

    def start(copy):
        copy.start()
        started.append(copy)
        return copy

    def hop_copy(s, n):
        part, distance, hop, dx = HOPS[n]
        dz = distance if s == 0 else NZ - distance
        unit = dz * NX + dx
        half = distance == NZ // 2
        if hop == 1:
            src = packed[part].at[unit, s] if half else packed[part].at[unit]
        elif half:
            src = relay_half[part].at[s, hop - 2, dx]
        else:
            src = relay[part].at[s, RELAY[distance, hop - 1], dx]
        if hop < distance:
            dst = relay_half[part].at[s, hop - 1, dx] if half else relay[part].at[s, RELAY[distance, hop], dx]
        else:
            dst = final[part].at[unit] if dx == 0 else turn[part].at[(dz - 1) * 3 + dx - 1]
            dst = dst.at[s] if half else dst
        return remote(src, dst, hop_send.at[s, n], hop_recv.at[s, n], (pool, at(0, 1 if s == 0 else NZ - 1)))

    hop_copies = [[hop_copy(s, n) for n in range(len(HOPS))] for s in range(2)]
    x_copies = {}

    def x_start(part, dz, dx, s):
        unit = dz * NX + dx
        src = packed[part].at[unit] if dz == 0 else turn[part].at[(dz - 1) * 3 + dx - 1]
        dst = final[part].at[unit]
        if dz == NZ // 2:
            src, dst = src.at[s], dst.at[s]
        sem = (dz * 3 + dx - 1) if s == 0 else 24 + dx - 1
        x_copies[part, dz, dx, s] = start(
            remote(src, dst, x_send.at[part, sem], x_recv.at[part, sem], (pool, at(dx, 0)))
        )

    def multiply(part, first, count, step):
        def one(i, carry):
            unit = first + i * step
            source = lax.rem(x + NX - lax.rem(unit, NX), NX) * NZ + lax.rem(z + NZ - unit // NX, NZ)
            total = None
            for rank in range(2):
                slot = table[1, source * 2 + rank]
                live = (slot >= 0) & (slot < count_in[0, 0])
                mine = bra[jnp.maximum(slot, 0)]
                mine = jnp.where(live, mine, jnp.zeros_like(mine))
                left = jnp.concatenate([mine[0], mine[1]], axis=1)
                ket = final[part][unit, rank]
                plain = jnp.concatenate([ket[0], ket[1]], axis=1)
                swapped = jnp.concatenate([ket[1], -ket[0]], axis=1)
                right = []
                for low in range(0, PARTS[part][1], GROUP):
                    right += [plain[low : low + GROUP], swapped[low : low + GROUP]]
                right = jnp.concatenate(right, axis=0)
                term = lax.dot_general(left, right, (((1,), (1,)), ((), ())), preferred_element_type=jnp.float32)
                total = term if total is None else total + term
            for group in range(PARTS[part][1] // GROUP):
                acc[part][group] += total[:, group * 128 : group * 128 + 128]
            return carry

        lax.fori_loop(0, count, one, 0)

    issued = [0, 0]
    position = {hop: n for n, hop in enumerate(HOPS)}

    def issue(s, arrived):
        while issued[s] < len(HOPS) and issued[s] <= arrived + WINDOW:
            part, distance, hop, dx = HOPS[issued[s]]
            if hop > 1 and position[part, distance, hop - 1, dx] > arrived:
                break
            start(hop_copies[s][issued[s]])
            issued[s] += 1

    for s in range(2):
        issue(s, -1)
    bra_copy = start(remote(coef, bra, bra_sem.at[0], bra_sem.at[1], (after, ga)))
    lax.fori_loop(0, 12, pack_unit, 0)
    lax.fori_loop(24, NX * NZ, pack_unit, 0)
    for part in range(2):
        final[part][0] = packed[part][0]
    count_copy = start(remote(count_out, count_in, count_sem.at[0], count_sem.at[1], (after, ga)))
    three = (2, 1, 3)
    for dx in three:
        x_start(0, 0, dx, 0)

    def wait_x(part, *dzs):
        for dz in dzs:
            for dx in three:
                for s in range(2 if dz == NZ // 2 else 1):
                    x_copies[part, dz, dx, s].wait_recv()

    def to_x():
        copies = []
        for dx in three:
            theirs = pl.ds(pl.multiple_of(lax.rem(x + dx, NX) * 64, 64), 64)
            copies.append(
                start(
                    remote(
                        acc[0].at[:, theirs],
                        x_in.at[dx - 1],
                        xr_send.at[dx - 1],
                        xr_recv.at[dx - 1],
                        (pool, at(dx, 0)),
                    )
                )
            )
        return copies

    def to_z():
        copies = []
        for dz in (4, 3, 5, 2, 6, 1, 7, 0):
            theirs = pl.ds(pl.multiple_of(lax.rem(z + dz, NZ) * 8, 8), 8)
            copies.append(
                start(remote(rows.at[:, theirs], z_in.at[dz], zr_send.at[dz], zr_recv.at[dz], (before, at(0, dz))))
            )
        return copies

    def when(part, distance, hop, dx):
        return position[part, distance, hop, dx]

    for n, (part, distance, hop, dx) in enumerate(HOPS):
        for s in range(2):
            hop_copies[s][n].wait_recv()
            if hop == distance and dx != 0:
                x_start(part, distance if s == 0 else NZ - distance, dx, s if distance == NZ // 2 else 0)
            issue(s, n)
        if n == 11:
            bra_copy.wait_recv()
            count_copy.wait_recv()
            wait_x(0, 0)
            multiply(0, 0, 4, 1)
            multiply(1, 0, 1, 1)
            for d in three:
                x_start(1, 0, d, 0)
        if n == 16:
            wait_x(0, 1, 7)
            multiply(0, 5, 3, 1)
            multiply(0, 29, 3, 1)
        if n == 26:
            wait_x(0, 2, 6)
            multiply(0, 9, 3, 1)
            multiply(0, 25, 3, 1)
            wait_x(1, 0)
            multiply(1, 1, 3, 1)
        if n == 32:
            wait_x(0, 3, 5)
            multiply(0, 13, 3, 1)
            multiply(0, 21, 3, 1)
        if n == 35:
            wait_x(0, 4)
            multiply(0, 17, 3, 1)
        if n == 37:
            multiply(0, 8, 2, 16)
        if n == 38:
            multiply(0, 12, 3, 4)
        if n == 39:
            multiply(0, 4, 2, 24)
            over_x = to_x()
        if n == when(1, 3, 1, 2):
            for copy in over_x:
                copy.wait_recv()
            own = pl.ds(pl.multiple_of(x * 64, 64), 64)
            rows[...] = acc[0][:, own] + x_in[0] + x_in[1] + x_in[2]
        if n == when(1, 3, 1, 1):
            over_z = to_z()
        if n == when(1, 3, 2, 2):
            wait_x(1, 1, 7)
            multiply(1, 5, 3, 1)
            multiply(1, 29, 3, 1)
        if n == when(1, 3, 3, 1):
            wait_x(1, 2, 6)
            multiply(1, 9, 3, 1)
            multiply(1, 25, 3, 1)
        if n == when(1, 3, 3, 0):
            wait_x(1, 3, 5)
            multiply(1, 12, 4, 1)
            multiply(1, 20, 4, 1)
        if n == when(1, 1, 1, 0):
            multiply(1, 4, 2, 24)
            wait_x(1, 4)
            multiply(1, 17, 3, 1)
        if n == when(1, 2, 2, 0):
            multiply(1, 8, 2, 16)
    multiply(1, 16, 1, 1)

    tails = []
    for dz in (4, 3, 5, 2, 6, 1, 7, 0):
        for dx in (2, 1, 3, 0):
            target = at(dx, dz)
            i = dz * NX + dx
            theirs = pl.ds(pl.multiple_of(target * 8, 8), 8)
            tails.append(
                start(
                    remote(acc[1].at[0, theirs], tail_in.at[i], tail_send.at[i], tail_recv.at[i], (before, target))
                )
            )
    for copy in over_z:
        copy.wait_recv()
    result = z_in[0]
    for dz in range(1, NZ):
        result = result + z_in[dz]
    for copy in tails:
        copy.wait_recv()
    last = tail_in[0]
    for i in range(1, NX * NZ):
        last = last + tail_in[i]
    groups = [result[0], result[1], result[2], last]
    for part in range(2):
        lanes = slice(part * GROUP, part * GROUP + GROUP)
        out_ref[part] = jnp.concatenate([group[:, lanes] for group in groups], axis=1) * norm_scale
    for copy in started:
        copy.wait_send()


def local(coefficients, stick_count, dest_device, dest_slot, source_stick):
    groups = lax.axis_size("ga")
    slots = coefficients.shape[1]
    bands = coefficients.shape[3]
    waves = coefficients.shape[4]
    norm_scale = (2 * groups * slots * waves) ** (-0.5)
    stick = (2, bands, waves)
    pieces = [(2, width, waves) for _, width in PARTS]
    bf16, f32 = jnp.bfloat16, jnp.float32
    dma = pltpu.SemaphoreType.DMA
    result = pl.pallas_call(
        functools.partial(kernel, norm_scale),
        out_shape=jax.ShapeDtypeStruct((2, bands // groups, bands), f32),
        in_specs=[
            pl.BlockSpec(memory_space=pl.ANY),
        ] * 5,
        out_specs=pl.BlockSpec(memory_space=pltpu.VMEM),
        scratch_shapes=[
            pltpu.VMEM((slots,) + stick, bf16),
            pltpu.VMEM((slots,) + stick, bf16),
            [pltpu.VMEM((1, width), jnp.int32) for width in (slots, slots, slots, 1)],
            pltpu.VMEM((8, 128), jnp.int32),
            pltpu.SMEM((8, 128), jnp.int32),
            pltpu.VMEM((8, 128), jnp.int32),
            pltpu.VMEM((8, 128), jnp.int32),
            [pltpu.VMEM((NX * NZ, 2) + piece, bf16) for piece in pieces],
            [pltpu.VMEM((2, 3, NX, 2) + piece, bf16) for piece in pieces],
            [pltpu.VMEM((2, 3, NX) + piece, bf16) for piece in pieces],
            [pltpu.VMEM((3 * (NZ - 1), 2) + piece, bf16) for piece in pieces],
            [pltpu.VMEM((NX * NZ, 2) + piece, bf16) for piece in pieces],
            [pltpu.VMEM((width // GROUP, bands, 128), f32) for _, width in PARTS],
            pltpu.VMEM((NX - 1, 3, bands // NX, 128), f32),
            pltpu.VMEM((3, bands // NX, 128), f32),
            pltpu.VMEM((NZ, 3, bands // groups, 128), f32),
            pltpu.VMEM((NX * NZ, bands // groups, 128), f32),
            dma,
            dma((4,)),
            dma,
            dma((2,)),
            dma((2,)),
            dma((2, len(HOPS))),
            dma((2, len(HOPS))),
            dma((2, 27)),
            dma((2, 27)),
            dma((NX - 1,)),
            dma((NX - 1,)),
            dma((NZ,)),
            dma((NZ,)),
            dma((NX * NZ,)),
            dma((NX * NZ,)),
        ],
        compiler_params=pltpu.CompilerParams(
            collective_id=0, has_side_effects=True, vmem_limit_bytes=56 * 2**20
        ),
    )(coefficients.reshape((slots,) + stick), stick_count, dest_device, dest_slot, source_stick)
    return result[None]


def solution(mesh):
    return jax.shard_map(
        local,
        mesh=mesh,
        in_specs=(
            P("pool", "ga", None, None, None),
            P("pool", "ga"),
            P("pool", "ga"),
            P("pool", "ga"),
            P("pool", "ga"),
        ),
        out_specs=P("pool", None, "ga", None),
        check_vma=False,
    )
```

```python
import functools

import jax
import jax.numpy as jnp
from jax import lax
from jax.experimental import pallas as pl
from jax.experimental.pallas import tpu as pltpu
from jax.sharding import PartitionSpec as P

MESH = pl.DeviceIdType.MESH
NX = 4
NZ = 8
WINDOW = 6
GROUP = 64
ALL = -1
PARTS = ((0, 192), (192, 64))


def hop_list():
    order = []

    def add(part, dxs, *hops):
        order.extend((part, distance, hop, dx) for distance, hop in hops for dx in dxs)

    far = (2, 1, 3)
    add(0, far, (4, 1), (3, 1), (1, 1), (2, 1), (4, 2), (3, 2), (2, 2), (4, 3), (3, 3), (4, 4))
    add(0, (0,), (4, 1), (3, 1), (2, 1), (4, 2), (3, 2), (2, 2), (4, 3), (3, 3), (4, 4), (1, 1))
    add(1, (ALL,), (1, 1), (4, 1), (3, 1), (2, 1), (4, 2), (3, 2), (2, 2))
    add(1, (0,), (4, 1))
    add(1, (ALL,), (4, 3))
    add(1, (0,), (3, 1))
    add(1, (ALL,), (3, 3))
    add(1, (0,), (4, 2), (3, 2))
    add(1, (ALL,), (4, 4))
    add(1, (0,), (2, 1), (4, 3), (3, 3), (1, 1), (2, 2), (4, 4))
    return order


HOPS = hop_list()
RELAY = {(2, 1): 0, (3, 1): 1, (3, 2): 2}


def kernel(
    norm_scale,
    coef_hbm,
    count_hbm,
    device_hbm,
    slot_hbm,
    source_hbm,
    out_ref,
    coef,
    bra,
    maps,
    tables,
    table,
    count_out,
    count_in,
    packed,
    relay,
    relay_half,
    turn,
    final,
    acc,
    x_in,
    rows,
    z_in,
    tail_in,
    load_sem,
    map_sem,
    table_sem,
    bra_sem,
    count_sem,
    hop_send,
    hop_recv,
    x_send,
    x_recv,
    xr_send,
    xr_recv,
    zr_send,
    zr_recv,
    tail_send,
    tail_recv,
):
    pool = lax.axis_index("pool")
    pools = lax.axis_size("pool")
    ga = lax.axis_index("ga")
    x = ga // NZ
    z = lax.rem(ga, NZ)
    after = lax.rem(pool + 1, pools)
    before = lax.rem(pool + pools - 1, pools)

    def at(dx, dz):
        return lax.rem(x + dx, NX) * NZ + lax.rem(z + dz, NZ)

    small = []
    for i, ref in enumerate((device_hbm, slot_hbm, source_hbm, count_hbm)):
        small.append(pltpu.make_async_copy(ref, maps[i], map_sem.at[i]))
        small[-1].start()
    load = pltpu.make_async_copy(coef_hbm, coef, load_sem)
    load.start()
    barrier = pltpu.get_barrier_semaphore()
    greeted = [(pool, at(0, 1)), (pool, at(0, NZ - 1))]
    greeted += [(pool, at(dx, 0)) for dx in range(1, NX)]
    greeted += [(before, ga)] + [(after, at(dx, dz)) for dz in range(NZ) for dx in range(NX)]
    for device in greeted:
        pl.semaphore_signal(barrier, inc=1, device_id=device, device_id_type=MESH)

    for copy in small:
        copy.wait()
    sent = maps[0][...]
    from_stick = maps[2][...]
    slots = sent.shape[1]
    upright = lax.broadcasted_iota(jnp.int32, (slots, slots), 0)
    across = lax.broadcasted_iota(jnp.int32, (slots, slots), 1)

    def standing(row):
        return jnp.sum(jnp.where(upright == across, row, 0), axis=1, keepdims=True)

    def rows_of(devices, order, missing):
        device, key = standing(devices), standing(order)
        earlier = (device == devices) & (order < key)
        rank = jnp.sum(earlier.astype(jnp.int32), axis=1, keepdims=True)
        row = jnp.where(device >= 0, device * 2 + rank, -1)
        lane = lax.broadcasted_iota(jnp.int32, (slots, 128), 1)
        stick = lax.broadcasted_iota(jnp.int32, (slots, 128), 0)
        return jnp.max(jnp.where(row == lane, stick, missing), axis=0, keepdims=True)

    tables[0:1] = rows_of(sent, maps[1][...], 0)
    tables[1:2] = rows_of(
        jnp.where(from_stick >= 0, from_stick // slots, -1), across[:1], -1
    )
    count_out[...] = jnp.broadcast_to(maps[3][...], count_out.shape)
    for total in acc:
        total[...] = jnp.zeros_like(total)
    to_scalars = pltpu.make_async_copy(tables, table, table_sem)
    to_scalars.start()
    load.wait()
    to_scalars.wait()

    def pack_unit(unit, carry):
        target = at(lax.rem(unit, NX), unit // NX)
        for rank in range(2):
            stick = coef[table[0, target * 2 + rank]]
            for part, (first, bands) in enumerate(PARTS):
                packed[part][unit, rank] = stick[:, first : first + bands]
        return carry

    lax.fori_loop(16, 20, pack_unit, 0)
    pl.semaphore_wait(barrier, len(greeted))

    def remote(src, dst, send, recv, device):
        return pltpu.make_async_remote_copy(
            src_ref=src, dst_ref=dst, send_sem=send, recv_sem=recv, device_id=device, device_id_type=MESH
        )

    started = []

    def start(copy):
        copy.start()
        started.append(copy)
        return copy

    def hop_copy(s, n):
        part, distance, hop, dx = HOPS[n]
        dz = distance if s == 0 else NZ - distance
        unit = dz * NX + dx
        lane, corner = dx, (dz - 1) * 3 + dx - 1
        if dx == ALL:
            unit, lane, corner = pl.ds(dz * NX + 1, 3), pl.ds(1, 3), pl.ds((dz - 1) * 3, 3)
        half = distance == NZ // 2
        if hop == 1:
            src = packed[part].at[unit, s] if half else packed[part].at[unit]
        elif half:
            src = relay_half[part].at[s, hop - 2, lane]
        else:
            src = relay[part].at[s, RELAY[distance, hop - 1], lane]
        if hop < distance:
            dst = relay_half[part].at[s, hop - 1, lane] if half else relay[part].at[s, RELAY[distance, hop], lane]
        else:
            over, place = (final, unit) if dx == 0 else (turn, corner)
            dst = over[part].at[place, s] if half else over[part].at[place]
        return remote(src, dst, hop_send.at[s, n], hop_recv.at[s, n], (pool, at(0, 1 if s == 0 else NZ - 1)))

    hop_copies = [[hop_copy(s, n) for n in range(len(HOPS))] for s in range(2)]
    x_copies = {}

    def x_start(part, dz, dx, s):
        unit = dz * NX + dx
        src = packed[part].at[unit] if dz == 0 else turn[part].at[(dz - 1) * 3 + dx - 1]
        dst = final[part].at[unit]
        if dz == NZ // 2:
            src, dst = src.at[s], dst.at[s]
        sem = (dz * 3 + dx - 1) if s == 0 else 24 + dx - 1
        x_copies[part, dz, dx, s] = start(
            remote(src, dst, x_send.at[part, sem], x_recv.at[part, sem], (pool, at(dx, 0)))
        )

    def multiply(part, first, count, step):
        def one(i, carry):
            unit = first + i * step
            source = lax.rem(x + NX - lax.rem(unit, NX), NX) * NZ + lax.rem(z + NZ - unit // NX, NZ)
            total = None
            for rank in range(2):
                slot = table[1, source * 2 + rank]
                live = (slot >= 0) & (slot < count_in[0, 0])
                mine = bra[jnp.maximum(slot, 0)]
                mine = jnp.where(live, mine, jnp.zeros_like(mine))
                left = jnp.concatenate([mine[0], mine[1]], axis=1)
                ket = final[part][unit, rank]
                plain = jnp.concatenate([ket[0], ket[1]], axis=1)
                swapped = jnp.concatenate([ket[1], -ket[0]], axis=1)
                right = []
                for low in range(0, PARTS[part][1], GROUP):
                    right += [plain[low : low + GROUP], swapped[low : low + GROUP]]
                right = jnp.concatenate(right, axis=0)
                term = lax.dot_general(left, right, (((1,), (1,)), ((), ())), preferred_element_type=jnp.float32)
                total = term if total is None else total + term
            for group in range(PARTS[part][1] // GROUP):
                acc[part][group] += total[:, group * 128 : group * 128 + 128]
            return carry

        lax.fori_loop(0, count, one, 0)

    issued = [0, 0]
    position = {hop: n for n, hop in enumerate(HOPS)}

    def issue(s, arrived):
        while issued[s] < len(HOPS) and issued[s] <= arrived + WINDOW:
            part, distance, hop, dx = HOPS[issued[s]]
            if hop > 1 and position[part, distance, hop - 1, dx] > arrived:
                break
            start(hop_copies[s][issued[s]])
            issued[s] += 1

    for s in range(2):
        for _ in range(3):
            start(hop_copies[s][issued[s]])
            issued[s] += 1
    lax.fori_loop(12, 16, pack_unit, 0)
    lax.fori_loop(20, 24, pack_unit, 0)
    lax.fori_loop(4, 8, pack_unit, 0)
    lax.fori_loop(28, 32, pack_unit, 0)
    for s in range(2):
        issue(s, -1)
    bra_copy = start(remote(coef, bra, bra_sem.at[0], bra_sem.at[1], (after, ga)))
    lax.fori_loop(0, 4, pack_unit, 0)
    lax.fori_loop(8, 12, pack_unit, 0)
    lax.fori_loop(24, 28, pack_unit, 0)
    for part in range(2):
        final[part][0] = packed[part][0]
    count_copy = start(remote(count_out, count_in, count_sem.at[0], count_sem.at[1], (after, ga)))
    three = (2, 1, 3)
    for dx in three:
        x_start(0, 0, dx, 0)

    def wait_x(part, *dzs):
        for dz in dzs:
            for dx in three:
                for s in range(2 if dz == NZ // 2 else 1):
                    x_copies[part, dz, dx, s].wait_recv()

    def to_x():
        copies = []
        for dx in three:
            theirs = pl.ds(pl.multiple_of(lax.rem(x + dx, NX) * 64, 64), 64)
            copies.append(
                start(
                    remote(
                        acc[0].at[:, theirs],
                        x_in.at[dx - 1],
                        xr_send.at[dx - 1],
                        xr_recv.at[dx - 1],
                        (pool, at(dx, 0)),
                    )
                )
            )
        return copies

    def to_z():
        copies = []
        for dz in (4, 3, 5, 2, 6, 1, 7, 0):
            theirs = pl.ds(pl.multiple_of(lax.rem(z + dz, NZ) * 8, 8), 8)
            copies.append(
                start(remote(rows.at[:, theirs], z_in.at[dz], zr_send.at[dz], zr_recv.at[dz], (before, at(0, dz))))
            )
        return copies

    def when(part, distance, hop, dx):
        return position[part, distance, hop, dx]

    for n, (part, distance, hop, dx) in enumerate(HOPS):
        for s in range(2):
            hop_copies[s][n].wait_recv()
            if hop == distance and dx != 0:
                for d in three if dx == ALL else (dx,):
                    x_start(part, distance if s == 0 else NZ - distance, d, s if distance == NZ // 2 else 0)
            issue(s, n)
        if n == 11:
            bra_copy.wait_recv()
            count_copy.wait_recv()
            wait_x(0, 0)
            multiply(0, 0, 4, 1)
            multiply(1, 0, 1, 1)
            for d in three:
                x_start(1, 0, d, 0)
        if n == 16:
            wait_x(0, 1, 7)
            multiply(0, 5, 3, 1)
            multiply(0, 29, 3, 1)
        if n == 26:
            wait_x(0, 2, 6)
            multiply(0, 9, 3, 1)
            multiply(0, 25, 3, 1)
            wait_x(1, 0)
            multiply(1, 1, 3, 1)
        if n == 32:
            wait_x(0, 3, 5)
            multiply(0, 13, 3, 1)
            multiply(0, 21, 3, 1)
        if n == 35:
            wait_x(0, 4)
            multiply(0, 17, 3, 1)
        if n == 37:
            multiply(0, 8, 2, 16)
        if n == 38:
            multiply(0, 12, 3, 4)
        if n == 39:
            multiply(0, 4, 2, 24)
            over_x = to_x()
        if n == when(1, 3, 1, ALL):
            for copy in over_x:
                copy.wait_recv()
            own = pl.ds(pl.multiple_of(x * 64, 64), 64)
            rows[...] = acc[0][:, own] + x_in[0] + x_in[1] + x_in[2]
        if n == when(1, 4, 4, ALL):
            over_z = to_z()
        if n == when(1, 3, 2, ALL):
            wait_x(1, 1, 7)
            multiply(1, 5, 3, 1)
            multiply(1, 29, 3, 1)
        if n == when(1, 3, 3, ALL):
            wait_x(1, 2, 6)
            multiply(1, 9, 3, 1)
            multiply(1, 25, 3, 1)
        if n == when(1, 3, 3, 0):
            wait_x(1, 3, 5)
            multiply(1, 12, 4, 1)
            multiply(1, 20, 4, 1)
        if n == when(1, 1, 1, 0):
            multiply(1, 4, 2, 24)
            wait_x(1, 4)
            multiply(1, 17, 3, 1)
        if n == when(1, 2, 2, 0):
            multiply(1, 8, 2, 16)
    multiply(1, 16, 1, 1)

    earlier = len(started)
    tails = []
    for dz in (4, 3, 5, 2, 6, 1, 7, 0):
        for dx in (2, 1, 3, 0):
            target = at(dx, dz)
            i = dz * NX + dx
            theirs = pl.ds(pl.multiple_of(target * 8, 8), 8)
            tails.append(
                start(
                    remote(acc[1].at[0, theirs], tail_in.at[i], tail_send.at[i], tail_recv.at[i], (before, target))
                )
            )
    for copy in started[:earlier]:
        copy.wait_send()
    for copy in over_z:
        copy.wait_recv()
    result = z_in[0]
    for dz in range(1, NZ):
        result = result + z_in[dz]
    for copy in tails:
        copy.wait_recv()
    last = tail_in[0]
    for i in range(1, NX * NZ):
        last = last + tail_in[i]
    groups = [result[0], result[1], result[2], last]
    for part in range(2):
        lanes = slice(part * GROUP, part * GROUP + GROUP)
        out_ref[part] = jnp.concatenate([group[:, lanes] for group in groups], axis=1)
    for copy in tails:
        copy.wait_send()


def local(coefficients, stick_count, dest_device, dest_slot, source_stick):
    groups = lax.axis_size("ga")
    slots = coefficients.shape[1]
    bands = coefficients.shape[3]
    waves = coefficients.shape[4]
    norm_scale = (2 * groups * slots * waves) ** (-0.5)
    stick = (2, bands, waves)
    pieces = [(2, width, waves) for _, width in PARTS]
    bf16, f32 = jnp.bfloat16, jnp.float32
    dma = pltpu.SemaphoreType.DMA
    result = pl.pallas_call(
        functools.partial(kernel, norm_scale),
        out_shape=jax.ShapeDtypeStruct((2, bands // groups, bands), f32),
        in_specs=[
            pl.BlockSpec(memory_space=pl.ANY),
        ] * 5,
        out_specs=pl.BlockSpec(memory_space=pltpu.VMEM),
        scratch_shapes=[
            pltpu.VMEM((slots,) + stick, bf16),
            pltpu.VMEM((slots,) + stick, bf16),
            [pltpu.VMEM((1, width), jnp.int32) for width in (slots, slots, slots, 1)],
            pltpu.VMEM((8, 128), jnp.int32),
            pltpu.SMEM((8, 128), jnp.int32),
            pltpu.VMEM((8, 128), jnp.int32),
            pltpu.VMEM((8, 128), jnp.int32),
            [pltpu.VMEM((NX * NZ, 2) + piece, bf16) for piece in pieces],
            [pltpu.VMEM((2, 3, NX, 2) + piece, bf16) for piece in pieces],
            [pltpu.VMEM((2, 3, NX) + piece, bf16) for piece in pieces],
            [pltpu.VMEM((3 * (NZ - 1), 2) + piece, bf16) for piece in pieces],
            [pltpu.VMEM((NX * NZ, 2) + piece, bf16) for piece in pieces],
            [pltpu.VMEM((width // GROUP, bands, 128), f32) for _, width in PARTS],
            pltpu.VMEM((NX - 1, 3, bands // NX, 128), f32),
            pltpu.VMEM((3, bands // NX, 128), f32),
            pltpu.VMEM((NZ, 3, bands // groups, 128), f32),
            pltpu.VMEM((NX * NZ, bands // groups, 128), f32),
            dma,
            dma((4,)),
            dma,
            dma((2,)),
            dma((2,)),
            dma((2, len(HOPS))),
            dma((2, len(HOPS))),
            dma((2, 27)),
            dma((2, 27)),
            dma((NX - 1,)),
            dma((NX - 1,)),
            dma((NZ,)),
            dma((NZ,)),
            dma((NX * NZ,)),
            dma((NX * NZ,)),
        ],
        compiler_params=pltpu.CompilerParams(
            collective_id=0, has_side_effects=True, vmem_limit_bytes=56 * 2**20
        ),
    )(coefficients.reshape((slots,) + stick), stick_count, dest_device, dest_slot, source_stick)
    return result[None] * norm_scale


def solution(mesh):
    return jax.shard_map(
        local,
        mesh=mesh,
        in_specs=(
            P("pool", "ga", None, None, None),
            P("pool", "ga"),
            P("pool", "ga"),
            P("pool", "ga"),
            P("pool", "ga"),
        ),
        out_specs=P("pool", None, "ga", None),
        check_vma=False,
    )
```

```python
import functools

import jax
import jax.numpy as jnp
from jax import lax
from jax.experimental import pallas as pl
from jax.experimental.pallas import tpu as pltpu
from jax.sharding import PartitionSpec as P

MESH = pl.DeviceIdType.MESH
NX = 4
NZ = 8
WINDOW = 6
GROUP = 64
ALL = -1
PARTS = ((0, 192), (192, 64))


def hop_list():
    order = []

    def add(part, dxs, *hops):
        order.extend((part, distance, hop, dx) for distance, hop in hops for dx in dxs)

    add(0, (ALL,), (4, 1), (3, 1), (1, 1), (2, 1), (4, 2), (3, 2), (2, 2), (4, 3), (3, 3), (4, 4))
    add(0, (0,), (4, 1), (3, 1), (2, 1), (4, 2), (3, 2), (2, 2), (4, 3), (3, 3), (4, 4), (1, 1))
    add(1, (ALL,), (1, 1), (4, 1), (3, 1), (2, 1), (4, 2), (3, 2), (2, 2))
    add(1, (0,), (4, 1))
    add(1, (ALL,), (4, 3))
    add(1, (0,), (3, 1))
    add(1, (ALL,), (3, 3))
    add(1, (0,), (4, 2), (3, 2))
    add(1, (ALL,), (4, 4))
    add(1, (0,), (2, 1), (4, 3), (3, 3), (1, 1), (2, 2), (4, 4))
    return order


HOPS = hop_list()
RELAY = {(2, 1): 0, (3, 1): 1, (3, 2): 2}


def kernel(
    norm_scale,
    coef_hbm,
    count_hbm,
    device_hbm,
    slot_hbm,
    source_hbm,
    out_ref,
    coef,
    bra,
    maps,
    tables,
    table,
    count_out,
    count_in,
    packed,
    relay,
    relay_half,
    turn,
    final,
    acc,
    x_in,
    rows,
    z_in,
    tail_in,
    load_sem,
    map_sem,
    table_sem,
    bra_sem,
    count_sem,
    hop_send,
    hop_recv,
    x_send,
    x_recv,
    xr_send,
    xr_recv,
    zr_send,
    zr_recv,
    tail_send,
    tail_recv,
):
    pool = lax.axis_index("pool")
    pools = lax.axis_size("pool")
    ga = lax.axis_index("ga")
    x = ga // NZ
    z = lax.rem(ga, NZ)
    after = lax.rem(pool + 1, pools)
    before = lax.rem(pool + pools - 1, pools)

    def at(dx, dz):
        return lax.rem(x + dx, NX) * NZ + lax.rem(z + dz, NZ)

    small = []
    for i, ref in enumerate((device_hbm, slot_hbm, source_hbm, count_hbm)):
        small.append(pltpu.make_async_copy(ref, maps[i], map_sem.at[i]))
        small[-1].start()
    load = pltpu.make_async_copy(coef_hbm, coef, load_sem)
    load.start()
    barrier = pltpu.get_barrier_semaphore()
    greeted = [(pool, at(0, 1)), (pool, at(0, NZ - 1))]
    greeted += [(pool, at(dx, 0)) for dx in range(1, NX)]
    greeted += [(before, ga)] + [(after, at(dx, dz)) for dz in range(NZ) for dx in range(NX)]
    for device in greeted:
        pl.semaphore_signal(barrier, inc=1, device_id=device, device_id_type=MESH)

    for copy in small:
        copy.wait()
    sent = maps[0][...]
    from_stick = maps[2][...]
    slots = sent.shape[1]
    upright = lax.broadcasted_iota(jnp.int32, (slots, slots), 0)
    across = lax.broadcasted_iota(jnp.int32, (slots, slots), 1)

    def standing(row):
        return jnp.sum(jnp.where(upright == across, row, 0), axis=1, keepdims=True)

    def rows_of(devices, order, missing):
        device, key = standing(devices), standing(order)
        earlier = (device == devices) & (order < key)
        rank = jnp.sum(earlier.astype(jnp.int32), axis=1, keepdims=True)
        row = jnp.where(device >= 0, device * 2 + rank, -1)
        lane = lax.broadcasted_iota(jnp.int32, (slots, 128), 1)
        stick = lax.broadcasted_iota(jnp.int32, (slots, 128), 0)
        return jnp.max(jnp.where(row == lane, stick, missing), axis=0, keepdims=True)

    tables[0:1] = rows_of(sent, maps[1][...], 0)
    tables[1:2] = rows_of(
        jnp.where(from_stick >= 0, from_stick // slots, -1), across[:1], -1
    )
    count_out[...] = jnp.broadcast_to(maps[3][...], count_out.shape)
    for total in acc:
        total[...] = jnp.zeros_like(total)
    to_scalars = pltpu.make_async_copy(tables, table, table_sem)
    to_scalars.start()
    load.wait()
    to_scalars.wait()

    def pack_unit(unit, carry):
        target = at(lax.rem(unit, NX), unit // NX)
        for rank in range(2):
            stick = coef[table[0, target * 2 + rank]]
            for part, (first, bands) in enumerate(PARTS):
                packed[part][unit, rank] = stick[:, first : first + bands]
        return carry

    lax.fori_loop(16, 20, pack_unit, 0)
    pl.semaphore_wait(barrier, len(greeted))

    def remote(src, dst, send, recv, device):
        return pltpu.make_async_remote_copy(
            src_ref=src, dst_ref=dst, send_sem=send, recv_sem=recv, device_id=device, device_id_type=MESH
        )

    started = []

    def start(copy):
        copy.start()
        started.append(copy)
        return copy

    def hop_copy(s, n):
        part, distance, hop, dx = HOPS[n]
        dz = distance if s == 0 else NZ - distance
        unit = dz * NX + dx
        lane, corner = dx, (dz - 1) * 3 + dx - 1
        if dx == ALL:
            unit, lane, corner = pl.ds(dz * NX + 1, 3), pl.ds(1, 3), pl.ds((dz - 1) * 3, 3)
        half = distance == NZ // 2
        if hop == 1:
            src = packed[part].at[unit, s] if half else packed[part].at[unit]
        elif half:
            src = relay_half[part].at[s, hop - 2, lane]
        else:
            src = relay[part].at[s, RELAY[distance, hop - 1], lane]
        if hop < distance:
            dst = relay_half[part].at[s, hop - 1, lane] if half else relay[part].at[s, RELAY[distance, hop], lane]
        else:
            over, place = (final, unit) if dx == 0 else (turn, corner)
            dst = over[part].at[place, s] if half else over[part].at[place]
        return remote(src, dst, hop_send.at[s, n], hop_recv.at[s, n], (pool, at(0, 1 if s == 0 else NZ - 1)))

    hop_copies = [[hop_copy(s, n) for n in range(len(HOPS))] for s in range(2)]
    x_copies = {}

    def x_start(part, dz, dx, s):
        unit = dz * NX + dx
        src = packed[part].at[unit] if dz == 0 else turn[part].at[(dz - 1) * 3 + dx - 1]
        dst = final[part].at[unit]
        if dz == NZ // 2:
            src, dst = src.at[s], dst.at[s]
        sem = (dz * 3 + dx - 1) if s == 0 else 24 + dx - 1
        x_copies[part, dz, dx, s] = start(
            remote(src, dst, x_send.at[part, sem], x_recv.at[part, sem], (pool, at(dx, 0)))
        )

    def multiply(part, first, count, step):
        def one(i, carry):
            unit = first + i * step
            source = lax.rem(x + NX - lax.rem(unit, NX), NX) * NZ + lax.rem(z + NZ - unit // NX, NZ)
            total = None
            for rank in range(2):
                slot = table[1, source * 2 + rank]
                live = (slot >= 0) & (slot < count_in[0, 0])
                mine = bra[jnp.maximum(slot, 0)]
                mine = jnp.where(live, mine, jnp.zeros_like(mine))
                left = jnp.concatenate([mine[0], mine[1]], axis=1)
                ket = final[part][unit, rank]
                plain = jnp.concatenate([ket[0], ket[1]], axis=1)
                swapped = jnp.concatenate([ket[1], -ket[0]], axis=1)
                right = []
                for low in range(0, PARTS[part][1], GROUP):
                    right += [plain[low : low + GROUP], swapped[low : low + GROUP]]
                right = jnp.concatenate(right, axis=0)
                term = lax.dot_general(left, right, (((1,), (1,)), ((), ())), preferred_element_type=jnp.float32)
                total = term if total is None else total + term
            for group in range(PARTS[part][1] // GROUP):
                acc[part][group] += total[:, group * 128 : group * 128 + 128]
            return carry

        lax.fori_loop(0, count, one, 0)

    issued = [0, 0]
    position = {hop: n for n, hop in enumerate(HOPS)}

    def issue(s, arrived):
        while issued[s] < len(HOPS) and issued[s] <= arrived + WINDOW:
            part, distance, hop, dx = HOPS[issued[s]]
            if hop > 1 and position[part, distance, hop - 1, dx] > arrived:
                break
            start(hop_copies[s][issued[s]])
            issued[s] += 1

    for s in range(2):
        for _ in range(1):
            start(hop_copies[s][issued[s]])
            issued[s] += 1
    lax.fori_loop(12, 16, pack_unit, 0)
    lax.fori_loop(20, 24, pack_unit, 0)
    lax.fori_loop(4, 8, pack_unit, 0)
    lax.fori_loop(28, 32, pack_unit, 0)
    lax.fori_loop(8, 12, pack_unit, 0)
    lax.fori_loop(24, 28, pack_unit, 0)
    for s in range(2):
        issue(s, -1)
    bra_copy = start(remote(coef, bra, bra_sem.at[0], bra_sem.at[1], (after, ga)))
    lax.fori_loop(0, 4, pack_unit, 0)
    for part in range(2):
        final[part][0] = packed[part][0]
    count_copy = start(remote(count_out, count_in, count_sem.at[0], count_sem.at[1], (after, ga)))
    three = (2, 1, 3)
    for dx in three:
        x_start(0, 0, dx, 0)

    def wait_x(part, *dzs):
        for dz in dzs:
            for dx in three:
                for s in range(2 if dz == NZ // 2 else 1):
                    x_copies[part, dz, dx, s].wait_recv()

    def to_x():
        copies = []
        for dx in three:
            theirs = pl.ds(pl.multiple_of(lax.rem(x + dx, NX) * 64, 64), 64)
            copies.append(
                start(
                    remote(
                        acc[0].at[:, theirs],
                        x_in.at[dx - 1],
                        xr_send.at[dx - 1],
                        xr_recv.at[dx - 1],
                        (pool, at(dx, 0)),
                    )
                )
            )
        return copies

    def to_z():
        copies = []
        for dz in (4, 3, 5, 2, 6, 1, 7, 0):
            theirs = pl.ds(pl.multiple_of(lax.rem(z + dz, NZ) * 8, 8), 8)
            copies.append(
                start(remote(rows.at[:, theirs], z_in.at[dz], zr_send.at[dz], zr_recv.at[dz], (before, at(0, dz))))
            )
        return copies

    def when(part, distance, hop, dx):
        return position[part, distance, hop, dx]

    for n, (part, distance, hop, dx) in enumerate(HOPS):
        for s in range(2):
            hop_copies[s][n].wait_recv()
            if hop == distance and dx != 0:
                for d in three if dx == ALL else (dx,):
                    x_start(part, distance if s == 0 else NZ - distance, d, s if distance == NZ // 2 else 0)
            issue(s, n)
        if n == 3:
            bra_copy.wait_recv()
            count_copy.wait_recv()
            wait_x(0, 0)
            multiply(0, 0, 4, 1)
            multiply(1, 0, 1, 1)
            for d in three:
                x_start(1, 0, d, 0)
        if n == 5:
            wait_x(0, 1, 7)
            multiply(0, 5, 3, 1)
            multiply(0, 29, 3, 1)
        if n == 8:
            wait_x(0, 2, 6)
            multiply(0, 9, 3, 1)
            multiply(0, 25, 3, 1)
            wait_x(1, 0)
            multiply(1, 1, 3, 1)
        if n == 12:
            wait_x(0, 3, 5)
            multiply(0, 13, 3, 1)
            multiply(0, 21, 3, 1)
        if n == 15:
            wait_x(0, 4)
            multiply(0, 17, 3, 1)
        if n == 17:
            multiply(0, 8, 2, 16)
        if n == 18:
            multiply(0, 12, 3, 4)
        if n == 19:
            multiply(0, 4, 2, 24)
            over_x = to_x()
        if n == when(1, 3, 1, ALL):
            for copy in over_x:
                copy.wait_recv()
            own = pl.ds(pl.multiple_of(x * 64, 64), 64)
            rows[...] = acc[0][:, own] + x_in[0] + x_in[1] + x_in[2]
        if n == when(1, 4, 4, ALL):
            over_z = to_z()
        if n == when(1, 3, 2, ALL):
            wait_x(1, 1, 7)
            multiply(1, 5, 3, 1)
            multiply(1, 29, 3, 1)
        if n == when(1, 3, 3, ALL):
            wait_x(1, 2, 6)
            multiply(1, 9, 3, 1)
            multiply(1, 25, 3, 1)
        if n == when(1, 3, 3, 0):
            wait_x(1, 3, 5)
            multiply(1, 12, 4, 1)
            multiply(1, 20, 4, 1)
        if n == when(1, 1, 1, 0):
            multiply(1, 4, 2, 24)
            wait_x(1, 4)
            multiply(1, 17, 3, 1)
        if n == when(1, 2, 2, 0):
            multiply(1, 8, 2, 16)
    multiply(1, 16, 1, 1)

    earlier = len(started)
    tails = []
    for dz in (4, 3, 5, 2, 6, 1, 7, 0):
        for dx in (2, 1, 3, 0):
            target = at(dx, dz)
            i = dz * NX + dx
            theirs = pl.ds(pl.multiple_of(target * 8, 8), 8)
            tails.append(
                start(
                    remote(acc[1].at[0, theirs], tail_in.at[i], tail_send.at[i], tail_recv.at[i], (before, target))
                )
            )
    for copy in started[:earlier]:
        copy.wait_send()
    for copy in over_z:
        copy.wait_recv()
    result = z_in[0]
    for dz in range(1, NZ):
        result = result + z_in[dz]
    for copy in tails:
        copy.wait_recv()
    last = tail_in[0]
    for i in range(1, NX * NZ):
        last = last + tail_in[i]
    groups = [result[0], result[1], result[2], last]
    for part in range(2):
        lanes = slice(part * GROUP, part * GROUP + GROUP)
        out_ref[part] = jnp.concatenate([group[:, lanes] for group in groups], axis=1)
    for copy in tails:
        copy.wait_send()


def local(coefficients, stick_count, dest_device, dest_slot, source_stick):
    groups = lax.axis_size("ga")
    slots = coefficients.shape[1]
    bands = coefficients.shape[3]
    waves = coefficients.shape[4]
    norm_scale = (2 * groups * slots * waves) ** (-0.5)
    stick = (2, bands, waves)
    pieces = [(2, width, waves) for _, width in PARTS]
    bf16, f32 = jnp.bfloat16, jnp.float32
    dma = pltpu.SemaphoreType.DMA
    result = pl.pallas_call(
        functools.partial(kernel, norm_scale),
        out_shape=jax.ShapeDtypeStruct((2, bands // groups, bands), f32),
        in_specs=[
            pl.BlockSpec(memory_space=pl.ANY),
        ] * 5,
        out_specs=pl.BlockSpec(memory_space=pltpu.VMEM),
        scratch_shapes=[
            pltpu.VMEM((slots,) + stick, bf16),
            pltpu.VMEM((slots,) + stick, bf16),
            [pltpu.VMEM((1, width), jnp.int32) for width in (slots, slots, slots, 1)],
            pltpu.VMEM((8, 128), jnp.int32),
            pltpu.SMEM((8, 128), jnp.int32),
            pltpu.VMEM((8, 128), jnp.int32),
            pltpu.VMEM((8, 128), jnp.int32),
            [pltpu.VMEM((NX * NZ, 2) + piece, bf16) for piece in pieces],
            [pltpu.VMEM((2, 3, NX, 2) + piece, bf16) for piece in pieces],
            [pltpu.VMEM((2, 3, NX) + piece, bf16) for piece in pieces],
            [pltpu.VMEM((3 * (NZ - 1), 2) + piece, bf16) for piece in pieces],
            [pltpu.VMEM((NX * NZ, 2) + piece, bf16) for piece in pieces],
            [pltpu.VMEM((width // GROUP, bands, 128), f32) for _, width in PARTS],
            pltpu.VMEM((NX - 1, 3, bands // NX, 128), f32),
            pltpu.VMEM((3, bands // NX, 128), f32),
            pltpu.VMEM((NZ, 3, bands // groups, 128), f32),
            pltpu.VMEM((NX * NZ, bands // groups, 128), f32),
            dma,
            dma((4,)),
            dma,
            dma((2,)),
            dma((2,)),
            dma((2, len(HOPS))),
            dma((2, len(HOPS))),
            dma((2, 27)),
            dma((2, 27)),
            dma((NX - 1,)),
            dma((NX - 1,)),
            dma((NZ,)),
            dma((NZ,)),
            dma((NX * NZ,)),
            dma((NX * NZ,)),
        ],
        compiler_params=pltpu.CompilerParams(
            collective_id=0, has_side_effects=True, vmem_limit_bytes=56 * 2**20
        ),
    )(coefficients.reshape((slots,) + stick), stick_count, dest_device, dest_slot, source_stick)
    return result[None] * norm_scale


def solution(mesh):
    return jax.shard_map(
        local,
        mesh=mesh,
        in_specs=(
            P("pool", "ga", None, None, None),
            P("pool", "ga"),
            P("pool", "ga"),
            P("pool", "ga"),
            P("pool", "ga"),
        ),
        out_specs=P("pool", None, "ga", None),
        check_vma=False,
    )
```
